32 devices in a mesh: img: 8 (over y, x, core), row: 4 (over z).
Axes of the slice: x: 2, y: 2, z: 4, core: 2. Of those that a mesh axis runs over, the one named last changes fastest.
Arguments:
- features: bfloat16 [8, 32, 384, 256], P('img', 'row'), may hold values from -6 to 6
- cotangent: bfloat16 [8, 32, 384, 256], P('img', 'row'), may hold values from -6 to 6
- weight_one: bfloat16 [3, 3, 256, 256], replicated, may hold values from -0.125 to 0.125
- weight_two: bfloat16 [3, 3, 256, 256], replicated, may hold values from -0.125 to 0.125
Outputs:
- input_grad: bfloat16 [8, 32, 384, 256], P('img', 'row')
- weight_one_grad: float32 [589824], P(('img', 'row'))
- weight_two_grad: float32 [589824], P(('img', 'row'))
The draws below stay inside these ranges and needn't reach their ends.
All inputs are finite; a program needn't handle non-finite values.
Results may differ from the reference program's by a relative error of at most 0.0055.
Values may be sent and summed in bfloat16 or wider, within the bound.
No kernel may reach another device: no remote copies, remote signals or barrier semaphores. Data moves between devices by JAX's collectives and lax.ppermute only.
A program may use at most 128 MiB of HBM per device.

```python
import math
import jax
import jax.numpy as jnp
from jax import lax

C = 256
COLS = 384
HEIGHT = 32
IMAGES = 8


def level_of(own_key, dims, cuts, smallest, top_value):
    def one(dim, parts):
        steps = jax.random.uniform(jax.random.fold_in(jax.random.fold_in(own_key, 6), dim), (parts,), jnp.float32, smallest / len(cuts), top_value / len(cuts))
        return jnp.repeat(jnp.exp(steps), dims[dim] // parts).reshape((-1,) + (1,) * (len(dims) - dim - 1))

    loudness = one(*cuts[0])
    for cut in cuts[1:]:
        loudness = loudness * one(*cut)
    return loudness


def scatter_about(stream_key, shape, spread, reach, split=(), held_as=jnp.bfloat16):
    factor_of = level_of(stream_key, shape, split, -0.22, 0.18) if split else 1.0
    array = jax.random.normal(stream_key, shape, jnp.float32) * spread * factor_of
    return jnp.minimum(jnp.maximum(array, -reach), reach).astype(held_as)


def setup_inputs(seed: int = 0) -> dict:
    arg_keys = jax.random.split(jax.random.key(seed), 5)
    return {
        "features": scatter_about(arg_keys[0], (IMAGES, HEIGHT, COLS, C), 1.0, 6.0, ((0, 8), (1, 4))),
        "cotangent": scatter_about(arg_keys[1], (IMAGES, HEIGHT, COLS, C), 1.0, 6.0, ((0, 8), (1, 4))),
        "weight_one": scatter_about(arg_keys[2], (3, 3, C, C), (9 * C) ** -0.5, 0.125),
        "weight_two": scatter_about(arg_keys[3], (3, 3, C, C), (9 * C) ** -0.5, 0.125),
    }


def gelu_slope(value):
    coeff = 0.7978845608028654
    tanhed = jnp.tanh(coeff * (value + 0.044715 * value * value * value))
    return 0.5 * (1.0 + tanhed) + 0.5 * value * (1.0 - tanhed * tanhed) * coeff * (1.0 + 3.0 * 0.044715 * value * value)

def widen(field):
    return jnp.pad(field, ((0, 0), (1, 1), (0, 0)))

def forward_taps(source, weight):
    rows = source.shape[0] - 2
    cols = source.shape[1]
    chans = source.shape[2]
    padded = widen(source)
    total = jnp.zeros((rows * cols, weight.shape[3]), jnp.float32)
    for tap_row in range(3):
        for tap_col in range(3):
            window = padded[tap_row:tap_row + rows, tap_col:tap_col + cols].reshape(rows * cols, chans)
            total = total + jnp.dot(window, weight[tap_row, tap_col], preferred_element_type=jnp.float32)
    return total.reshape(rows, cols, weight.shape[3])

def backward_taps(source, weight):
    rows = source.shape[0] - 2
    cols = source.shape[1]
    chans = source.shape[2]
    padded = widen(source)
    total = jnp.zeros((rows * cols, weight.shape[2]), jnp.float32)
    for tap_row in range(3):
        for tap_col in range(3):
            window = padded[2 - tap_row:2 - tap_row + rows, 2 - tap_col:2 - tap_col + cols].reshape(rows * cols, chans)
            total = total + lax.dot_general(window, weight[tap_row, tap_col], (((1,), (1,)), ((), ())), preferred_element_type=jnp.float32)
    return total.reshape(rows, cols, weight.shape[2])

def weight_taps(source, grads, offset):
    rows = grads.shape[0]
    cols = grads.shape[1]
    chans = source.shape[2]
    padded = widen(source)
    flat_grads = grads.reshape(rows * cols, grads.shape[2])
    pieces = []
    for tap_row in range(3):
        for tap_col in range(3):
            window = padded[offset + tap_row:offset + tap_row + rows, tap_col:tap_col + cols].reshape(rows * cols, chans)
            pieces.append(lax.dot_general(window, flat_grads, (((0,), (0,)), ((), ())), preferred_element_type=jnp.float32))
    return jnp.stack(pieces)

def local_pass(inputs_wide, grads_wide, inside, weight_one, weight_two):
    rows = inputs_wide.shape[0] - 4
    acted = jax.nn.gelu(inputs_wide.astype(jnp.float32), approximate=True).astype(jnp.bfloat16)
    hidden = forward_taps(acted, weight_one)
    middle = inside[1:rows + 3][:, None, None]
    gated = (jax.nn.gelu(hidden, approximate=True) * middle).astype(jnp.bfloat16)
    back_hidden = backward_taps(grads_wide, weight_two)
    hidden_grad = (back_hidden * gelu_slope(hidden) * middle).astype(jnp.bfloat16)
    back_input = backward_taps(hidden_grad, weight_one)
    own_inputs = inputs_wide[2:rows + 2].astype(jnp.float32)
    own_grads = grads_wide[2:rows + 2]
    input_grad = (own_grads.astype(jnp.float32) + back_input * gelu_slope(own_inputs)).astype(jnp.bfloat16)
    grad_two = weight_taps(gated, own_grads, 0)
    grad_one = weight_taps(acted, hidden_grad[1:rows + 1], 1)
    return (input_grad, grad_one, grad_two)

def reference(features, cotangent, weight_one, weight_two):
    height = features.shape[1]
    chans = features.shape[3]
    places = jnp.arange(height + 4)
    inside = ((places >= 2) & (places < height + 2)).astype(jnp.float32)

    def per_image(carry, pair):
        inputs, grads = pair
        inputs_wide = jnp.pad(inputs, ((2, 2), (0, 0), (0, 0)))
        grads_wide = jnp.pad(grads, ((2, 2), (0, 0), (0, 0)))
        input_grad, grad_one, grad_two = local_pass(inputs_wide, grads_wide, inside, weight_one, weight_two)
        return ((carry[0] + grad_one, carry[1] + grad_two), input_grad)
    empty = jnp.zeros((9, chans, chans), jnp.float32)
    totals, input_grads = lax.scan(per_image, (empty, empty), (features, cotangent))
    scale = 1.0 / math.sqrt(features.shape[0] * height * features.shape[2])
    return (input_grads, (totals[0] * scale).reshape(-1), (totals[1] * scale).reshape(-1))
```

```python
import functools
import math

import jax
import jax.numpy as jnp
from jax import lax
from jax.experimental import pallas as pl
from jax.experimental.pallas import tpu as pltpu
from jax.sharding import PartitionSpec as P

COEFF = 0.7978845608028654
CUBE = 0.044715
F32 = jnp.float32
BF16 = jnp.bfloat16
VMEM = pl.BlockSpec(memory_space=pltpu.VMEM)
NT = (((1,), (1,)), ((), ()))


def gelu_parts(value):
    square = value * value
    tanhed = jnp.tanh(value * (COEFF + (COEFF * CUBE) * square))
    half = 0.5 + 0.5 * tanhed
    return (square, half, value * half)


def gelu_slope(square, half, gated):
    return half + gated * (1.0 - half) * (2.0 * COEFF + (6.0 * COEFF * CUBE) * square)


def column_shifts(field):
    cols = field.shape[0]
    spot = lax.broadcasted_iota(jnp.int32, field.shape, 0)
    left = jnp.where(spot == 0, 0.0, pltpu.roll(field, 1, 0))
    right = jnp.where(spot == cols - 1, 0.0, pltpu.roll(field, cols - 1, 0))
    return (left.astype(BF16), field.astype(BF16), right.astype(BF16))


def hidden_kernel(rows, cols, chans, block, f_ref, c_ref, w1_ref, w2_ref, hg_ref, at_ref, g2_ref, x3, c3, gt):
    def prepare(r, carry):
        base = pl.multiple_of(r * cols, cols)
        _, _, acted = gelu_parts(f_ref[r].astype(F32))
        left, mid, right = column_shifts(acted)
        x3[pl.ds(base, cols), 0:chans] = left
        x3[pl.ds(base, cols), chans : 2 * chans] = mid
        x3[pl.ds(base, cols), 2 * chans : 3 * chans] = right
        at_ref[:, pl.ds(base, cols)] = mid.T
        left, mid, right = column_shifts(c_ref[r].astype(F32))
        c3[pl.ds(base, cols), 0:chans] = right
        c3[pl.ds(base, cols), chans : 2 * chans] = mid
        c3[pl.ds(base, cols), 2 * chans : 3 * chans] = left
        return carry

    lax.fori_loop(0, rows + 2, prepare, 0)
    size = block * cols

    def convolve(step, carry):
        hidden = jnp.zeros((size, chans), F32)
        back = jnp.zeros((size, chans), F32)
        for a in range(3):
            ahead = pl.multiple_of((step * block + a) * cols, cols)
            behind = pl.multiple_of((step * block + 2 - a) * cols, cols)
            for b in range(3):
                part = slice(b * chans, (b + 1) * chans)
                hidden += jnp.dot(x3[pl.ds(ahead, size), part], w1_ref[a, b], preferred_element_type=F32)
                back += lax.dot_general(c3[pl.ds(behind, size), part], w2_ref[a, b], NT, preferred_element_type=F32)
        square, half, gated = gelu_parts(hidden)
        base = pl.multiple_of(step * size, size)
        gt[:, pl.ds(base, size)] = gated.astype(BF16).T
        hg_ref[pl.ds(base, size), :] = (back * gelu_slope(square, half, gated)).astype(BF16)
        return carry

    lax.fori_loop(0, rows // block, convolve, 0)
    for a in range(3):
        for b in range(3):
            g2_ref[a, b] = jnp.dot(
                gt[...], c3[(2 - a) * cols : (2 - a + rows) * cols, b * chans : (b + 1) * chans],
                preferred_element_type=F32,
            ).astype(BF16)


def grad_kernel(rows, cols, chans, hg_ref, at_ref, g1_ref, h3_ref):
    def prepare(r, carry):
        base = pl.multiple_of(r * cols, cols)
        left, mid, right = column_shifts(hg_ref[pl.ds(base, cols), :].astype(F32))
        h3_ref[pl.ds(base, cols), 0:chans] = right
        h3_ref[pl.ds(base, cols), chans : 2 * chans] = mid
        h3_ref[pl.ds(base, cols), 2 * chans : 3 * chans] = left
        return carry

    lax.fori_loop(0, rows, prepare, 0)
    for a in range(3):
        for b in range(3):
            g1_ref[a, b] = jnp.dot(
                at_ref[:, a * cols : (a + rows) * cols], h3_ref[:, b * chans : (b + 1) * chans],
                preferred_element_type=F32,
            ).astype(BF16)


def input_kernel(rows, cols, chans, block, h3_ref, top_ref, low_ref, f_ref, c_ref, w1_ref, out_ref, h3):
    h3[cols : (rows + 1) * cols, :] = h3_ref[...]
    for ref, r in ((top_ref, 0), (low_ref, rows + 1)):
        left, mid, right = column_shifts(ref[...].astype(F32))
        h3[r * cols : (r + 1) * cols, 0:chans] = right
        h3[r * cols : (r + 1) * cols, chans : 2 * chans] = mid
        h3[r * cols : (r + 1) * cols, 2 * chans : 3 * chans] = left
    size = block * cols

    def convolve(step, carry):
        back = jnp.zeros((size, chans), F32)
        for a in range(3):
            behind = pl.multiple_of((step * block + 2 - a) * cols, cols)
            for b in range(3):
                part = slice(b * chans, (b + 1) * chans)
                back += lax.dot_general(h3[pl.ds(behind, size), part], w1_ref[a, b], NT, preferred_element_type=F32)
        here = pl.ds(pl.multiple_of(step * size, size), size)
        slope = gelu_slope(*gelu_parts(f_ref[here, :].astype(F32)))
        out_ref[here, :] = (c_ref[here, :].astype(F32) + back * slope).astype(BF16)
        return carry

    lax.fori_loop(0, rows // block, convolve, 0)


def exchange(flat, axis):
    peers = lax.axis_size(axis)
    parts = flat.reshape(peers, flat.shape[0] // peers, flat.shape[1])
    parts = lax.all_to_all(parts, axis, 0, 0)
    return jnp.sum(parts.astype(F32), axis=0)


def shards(features, cotangent, weight_one, weight_two):
    _, rows, cols, chans = features.shape
    peers = lax.axis_size("row")
    height = rows * peers
    down = [(i, i + 1) for i in range(peers - 1)]
    up = [(j, i) for i, j in down]
    both = jnp.stack([features[0], cotangent[0]])
    before = lax.ppermute(both[:, rows - 1 :], "row", down)
    after = lax.ppermute(both[:, :1], "row", up)
    wide = jnp.concatenate([before, both, after], axis=1)
    block = 4
    shape = jax.ShapeDtypeStruct
    cells = rows * cols
    hidden_grad, acted_t, grad_two = pl.pallas_call(
        functools.partial(hidden_kernel, rows, cols, chans, block),
        out_shape=(
            shape((cells, chans), BF16),
            shape((chans, cells + 2 * cols), BF16),
            shape((3, 3, chans, chans), BF16),
        ),
        in_specs=[VMEM] * 4,
        out_specs=[VMEM] * 3,
        scratch_shapes=[
            pltpu.VMEM((cells + 2 * cols, 3 * chans), BF16),
            pltpu.VMEM((cells + 2 * cols, 3 * chans), BF16),
            pltpu.VMEM((chans, cells), BF16),
        ],
        name="hidden",
    )(wide[0], wide[1], weight_one, weight_two)
    top = lax.ppermute(hidden_grad[cells - cols :], "row", down)
    low = lax.ppermute(hidden_grad[:cols], "row", up)
    grad_one, hidden_shifts = pl.pallas_call(
        functools.partial(grad_kernel, rows, cols, chans),
        out_shape=(shape((3, 3, chans, chans), BF16), shape((cells, 3 * chans), BF16)),
        in_specs=[VMEM] * 2,
        out_specs=[VMEM] * 2,
        name="grad",
    )(hidden_grad, acted_t)
    input_grad = pl.pallas_call(
        functools.partial(input_kernel, rows, cols, chans, block),
        out_shape=shape((cells, chans), BF16),
        in_specs=[VMEM] * 6,
        out_specs=VMEM,
        scratch_shapes=[pltpu.VMEM((cells + 2 * cols, 3 * chans), BF16)],
        name="input",
    )(hidden_shifts, top, low, features.reshape(cells, chans), cotangent.reshape(cells, chans), weight_one)
    scale = 1.0 / math.sqrt(lax.axis_size("img") * height * cols)
    outs = []
    for grad in (grad_one, grad_two):
        part = exchange(grad.reshape(9 * chans, chans), "img").astype(BF16)
        outs.append((exchange(part, "row") * scale).reshape(-1))
    return (input_grad.reshape(features.shape), outs[0], outs[1])


def solution(mesh):
    placed = (P("img", "row", None, None), P("img", "row", None, None), P(), P())
    return jax.shard_map(
        shards,
        mesh=mesh,
        in_specs=placed,
        out_specs=(P("img", "row", None, None), P(("img", "row")), P(("img", "row"))),
        check_vma=False,
    )
```

```python
import functools
import math

import jax
import jax.numpy as jnp
from jax import lax
from jax.experimental import pallas as pl
from jax.experimental.pallas import tpu as pltpu
from jax.sharding import PartitionSpec as P


COEFF = 0.7978845608028654
CUBE = 0.044715
F32 = jnp.float32
BF16 = jnp.bfloat16
VMEM = pl.BlockSpec(memory_space=pltpu.VMEM)
SMEM = pl.BlockSpec(memory_space=pltpu.SMEM)
NN = (((1,), (0,)), ((), ()))
NT = (((1,), (1,)), ((), ()))
MIB = 1024 * 1024


def gelu_parts(value):
    square = value * value
    tanhed = jnp.tanh(value * (COEFF + (COEFF * CUBE) * square))
    half = 0.5 + 0.5 * tanhed
    return (square, half, value * half)


def gelu_slope(square, half, gated):
    return half + gated * (1.0 - half) * (2.0 * COEFF + (6.0 * COEFF * CUBE) * square)


def column_shifts(field):
    cols = field.shape[0]
    spot = lax.broadcasted_iota(jnp.int32, field.shape, 0)
    left = jnp.where(spot == 0, 0.0, pltpu.roll(field, 1, 0))
    right = jnp.where(spot == cols - 1, 0.0, pltpu.roll(field, cols - 1, 0))
    return (left.astype(BF16), field.astype(BF16), right.astype(BF16))


def put_shifts(ref, base, cols, shifts):
    chans = shifts[0].shape[1]
    for b, value in enumerate(shifts):
        ref[pl.ds(base, cols), b * chans : (b + 1) * chans] = value


def dot(left, right, dims=NN):
    return lax.dot_general(left, right, dims, preferred_element_type=F32)


def conv(windows, weight, dims):
    chans = weight.shape[-1]
    total = None
    for a in range(3):
        for b in range(3):
            part = slice(b * chans, (b + 1) * chans)
            terms = [dot(ref[start : start + length, part], weight[a, b], dims) for ref, start, length in windows[a]]
            term = terms[0] if len(terms) == 1 else jnp.concatenate(terms, axis=0)
            total = term if total is None else total + term
    return total


def window(own, top, low, first, count, rows, cols):
    pieces = []
    if first < 0:
        pieces.append((top, 0, cols))
    begin, end = max(first, 0), min(first + count, rows)
    if end > begin:
        pieces.append((own, begin * cols, (end - begin) * cols))
    if first + count > rows:
        pieces.append((low, 0, cols))
    return pieces


def is_even():
    return lax.axis_index("row") % 2 == 0


def pack_kernel(f_first, f_last, c_first, c_last, to_a, to_b):
    even = is_even()
    for i, (head, tail) in enumerate(((f_first, f_last), (c_first, c_last))):
        to_a[i] = jnp.where(even, tail[...], head[...])
        to_b[i] = jnp.where(even, head[...], tail[...])


def inner_kernel(rows, cols, f_ref, c_ref, w1_ref, x3, c3, at, gt, slope):
    def prepare(r, carry):
        base = pl.multiple_of(r * cols, cols)
        acted = gelu_parts(f_ref[pl.ds(base, cols), :].astype(F32))[2]
        shifts = column_shifts(acted)
        put_shifts(x3, base, cols, shifts)
        at[:, pl.ds(base, cols)] = shifts[1].T
        put_shifts(c3, base, cols, column_shifts(c_ref[pl.ds(base, cols), :].astype(F32))[::-1])
        return carry

    lax.fori_loop(0, rows, prepare, 0)
    block = (rows - 2) // 2
    for first in (1, 1 + block):
        hidden = conv([window(x3, None, None, first - 1 + a, block, rows, cols) for a in range(3)], w1_ref, NN)
        parts = gelu_parts(hidden)
        here = slice((first - 1) * cols, (first - 1 + block) * cols)
        gt[:, here] = parts[2].astype(BF16).T
        slope[here, :] = gelu_slope(*parts)


def place(box, value, tap):
    core, chip, size = lax.axis_index("img") % 2, lax.axis_index("img") // 2, box.shape[2]
    start = tap * value.shape[0]
    row = start
    while row < start + value.shape[0]:
        index, offset = divmod(row, size)
        count = min(size - offset, start + value.shape[0] - row)
        box[(index % 2) ^ core, (index // 2) ^ chip, offset : offset + count, :] = value[
            row - start : row - start + count
        ].astype(BF16)
        row += count


def edge_kernel(
    rows, cols, fc_a, fc_b, x3, c3, w1_ref, gt, top3, low3, at_edge, slope, own, other, xe, ge, box
):
    even = is_even()
    for e in range(2):
        halo = [jnp.where(even, (fc_b, fc_a)[e][i], (fc_a, fc_b)[e][i]) for i in range(2)]
        acted = gelu_parts(halo[0].astype(F32))[2]
        shifts = column_shifts(acted)
        put_shifts(xe, e * cols, cols, shifts)
        at_edge[:, e * cols : (e + 1) * cols] = shifts[1].T
        put_shifts((top3, low3)[e], 0, cols, column_shifts(halo[1].astype(F32))[::-1])
    xtop, xlow = xe.at[0:cols], xe.at[cols : 2 * cols]
    for e, row in enumerate((0, rows - 1)):
        hidden = conv([window(x3, xtop, xlow, row - 1 + a, 1, rows, cols) for a in range(3)], w1_ref, NN)
        parts = gelu_parts(hidden)
        here = slice(e * cols, (e + 1) * cols)
        ge[:, here] = parts[2].astype(BF16).T
        slope[here, :] = gelu_slope(*parts)
    chans = w1_ref.shape[-1]
    for a in range(3):
        for b in range(3):
            part = slice(b * chans, (b + 1) * chans)
            total = dot(gt[...], c3[(2 - a) * cols : (rows - a) * cols, part])
            for e, row in enumerate((1 - a, rows - a)):
                ((ref, start, length),) = window(c3, top3, low3, row, 1, rows, cols)
                total += dot(ge[:, e * cols : (e + 1) * cols], ref[start : start + length, part])
            place(box, total, 3 * a + b)
    own[...] = box[0]
    other[...] = box[1]


def back_kernel(rows, cols, c3, top3, low3, w2_ref, slope, slope_edge, to_a, to_b, h3):
    block = rows // 2
    even = is_even()
    for first in (0, block):
        back = conv([window(c3, top3, low3, first + 1 - a, block, rows, cols) for a in range(3)], w2_ref, NT)
        for i in range(block):
            row = first + i
            if row == 0:
                factor = slope_edge[0:cols, :]
            elif row == rows - 1:
                factor = slope_edge[cols : 2 * cols, :]
            else:
                factor = slope[(row - 1) * cols : row * cols, :]
            value = (back[i * cols : (i + 1) * cols] * factor).astype(BF16)
            if row == 0:
                head = value
            if row == rows - 1:
                to_a[...] = jnp.where(even, value, head)
                to_b[...] = jnp.where(even, head, value)
            put_shifts(h3, row * cols, cols, column_shifts(value.astype(F32))[::-1])


def grad_kernel(rows, cols, at, at_edge, h3, own, other, box):
    chans = at.shape[0]
    for a in range(3):
        for b in range(3):
            part = slice(b * chans, (b + 1) * chans)
            if a == 1:
                total = dot(at[...], h3[:, part])
            elif a == 0:
                total = dot(at[:, : (rows - 1) * cols], h3[cols:, part])
                total += dot(at_edge[:, :cols], h3[:cols, part])
            else:
                total = dot(at[:, cols:], h3[: (rows - 1) * cols, part])
                total += dot(at_edge[:, cols:], h3[(rows - 1) * cols :, part])
            place(box, total, 3 * a + b)
    own[...] = box[0]
    other[...] = box[1]


def input_kernel(rows, cols, first, h3, got_a, got_b, f_ref, c_ref, w1_ref, *rest):
    out_ref, edge3 = rest[-2:]
    block = rows // 2
    even = is_even() if first == 0 else jnp.logical_not(is_even())
    halo = jnp.where(even, got_b[...], got_a[...])
    put_shifts(edge3, 0, cols, column_shifts(halo.astype(F32))[::-1])
    back = conv([window(h3, edge3, edge3, first + 1 - a, block, rows, cols) for a in range(3)], w1_ref, NT)
    here = slice(first * cols, (first + block) * cols)
    slope = gelu_slope(*gelu_parts(f_ref[here, :].astype(F32)))
    out_ref[...] = (c_ref[here, :].astype(F32) + back * slope).astype(BF16)


def pair_kernel(blocks, own, other, *outs):
    for k in range(blocks):
        outs[k][...] = (own[k].astype(F32) + other[k].astype(F32)).astype(BF16)


def chip_kernel(blocks, peers, *refs):
    terms, outs, whole, cut = refs[: 2 * blocks], refs[2 * blocks : 2 * blocks + peers], refs[-2], refs[-1]
    size = cut.shape[1]
    for g in range(2):
        total = terms[g * blocks][...].astype(F32)
        for k in range(1, blocks):
            total += terms[g * blocks + k][...].astype(F32)
        whole[...] = total
        for k in range(peers):
            cut[k] = whole[k * size : (k + 1) * size, :]
        for k in range(peers):
            outs[k][g] = cut[lax.axis_index("row") ^ k].astype(BF16)


def last_kernel(peers, scale, *refs):
    terms, outs = refs[:peers], refs[peers:]
    for g in range(2):
        total = terms[0][g].astype(F32)
        for k in range(1, peers):
            total += terms[k][g].astype(F32)
        total = total * scale
        size = total.shape[0]
        outs[g][pl.ds(0, size, stride=2), :] = total[:, :128]
        outs[g][pl.ds(1, size, stride=2), :] = total[:, 128:]


def call(kernel, outs, operands, scratch=(), flops=0, limit=24, specs=None, **extra):
    out_shape = tuple(jax.ShapeDtypeStruct(shape, dtype) for shape, dtype in outs)
    moved = sum(math.prod(shape) * jnp.dtype(dtype).itemsize for shape, dtype in outs)
    moved += sum(operand.size * operand.dtype.itemsize for operand in operands)
    return pl.pallas_call(
        kernel,
        out_shape=out_shape,
        in_specs=specs or [VMEM] * len(operands),
        out_specs=extra.pop("out_specs", tuple([VMEM] * len(outs))),
        scratch_shapes=list(scratch),
        cost_estimate=pl.CostEstimate(flops=flops, bytes_accessed=moved, transcendentals=0),
        compiler_params=pltpu.CompilerParams(vmem_limit_bytes=limit * MIB),
        **extra,
    )(*operands)


def flip(axis, bits):
    return [(i, i ^ bits) for i in range(lax.axis_size(axis))]


def neighbours(start, peers):
    pairs = [(i, i + 1) for i in range(start, peers - 1, 2)]
    return pairs + [(j, i) for i, j in pairs]


def local_part(features, cotangent, weight_one, weight_two):
    _, rows, cols, chans = features.shape
    peers = lax.axis_size("row")
    images = lax.axis_size("img")
    blocks = images // 2
    height = rows * peers
    cells = rows * cols
    size = 9 * chans // images
    cut = size // peers
    pairs_a, pairs_b = neighbours(0, peers), neighbours(1, peers)
    f_own = features.reshape(cells, chans)
    c_own = cotangent.reshape(cells, chans)
    ends = [pl.BlockSpec((cols, chans), lambda i, row=row: (row, 0)) for row in (0, rows - 1)]
    to_a, to_b = call(
        pack_kernel, [((2, cols, chans), BF16)] * 2, (f_own, f_own, c_own, c_own), specs=ends * 2, grid=(1,),
    )
    fc_a = lax.ppermute(to_a, "row", pairs_a)
    fc_b = lax.ppermute(to_b, "row", pairs_b)
    unit = 2 * cells * 9 * chans * chans
    wide = (cells, 3 * chans)
    pair = [((blocks, size, chans), BF16)] * 2
    box = pltpu.VMEM((2, blocks, size, chans), BF16)
    inner_cells = cells - 2 * cols
    sums = [((size, chans), BF16)] * blocks

    x3, c3, at, gt, slope = call(
        functools.partial(inner_kernel, rows, cols),
        [(wide, BF16), (wide, BF16), ((chans, cells), BF16), ((chans, inner_cells), BF16), ((inner_cells, chans), F32)],
        (f_own, c_own, weight_one), flops=unit,
    )
    top3, low3, at_edge, slope_edge, own_two, other_two = call(
        functools.partial(edge_kernel, rows, cols),
        [((cols, 3 * chans), BF16)] * 2 + [((chans, 2 * cols), BF16), ((2 * cols, chans), F32)] + pair,
        (fc_a, fc_b, x3, c3, weight_one, gt),
        scratch=[pltpu.VMEM((2 * cols, 3 * chans), BF16), pltpu.VMEM((chans, 2 * cols), BF16), box],
        flops=unit + unit // 4,
    )
    got_two = lax.ppermute(other_two, "img", flip("img", 1))
    to_a, to_b, h3 = call(
        functools.partial(back_kernel, rows, cols),
        [((cols, chans), BF16)] * 2 + [(wide, BF16)],
        (c3, top3, low3, weight_two, slope, slope_edge), flops=unit,
    )
    hg_a = lax.ppermute(to_a, "row", pairs_a)
    hg_b = lax.ppermute(to_b, "row", pairs_b)
    sums_two = call(functools.partial(pair_kernel, blocks), sums, (own_two, got_two))
    terms_two = [sums_two[0]]
    terms_two += [lax.ppermute(sums_two[k], "img", flip("img", 2 * k)) for k in range(1, blocks)]
    own_one, other_one = call(
        functools.partial(grad_kernel, rows, cols), pair, (at, at_edge, h3), scratch=[box], flops=unit,
    )
    got_one = lax.ppermute(other_one, "img", flip("img", 1))
    result = ()
    for part in range(2):
        result = call(
            functools.partial(input_kernel, rows, cols, part * (rows // 2)), [((cells, chans), BF16)],
            (h3, hg_a, hg_b, f_own, c_own, weight_one, *result), flops=unit // 2,
            scratch=[pltpu.VMEM((cols, 3 * chans), BF16)], grid=(1,),
            specs=[VMEM] * 6 + [pl.BlockSpec(memory_space=pl.ANY)] * part,
            out_specs=(pl.BlockSpec((cells // 2, chans), lambda i, part=part: (part, 0)),),
            input_output_aliases={6: 0} if part else {},
        )
    sums_one = call(functools.partial(pair_kernel, blocks), sums, (own_one, got_one))
    terms_one = [sums_one[0]]
    terms_one += [lax.ppermute(sums_one[k], "img", flip("img", 2 * k)) for k in range(1, blocks)]
    cuts = call(
        functools.partial(chip_kernel, blocks, peers), [((2, cut, chans), BF16)] * peers,
        (*terms_one, *terms_two),
        scratch=[pltpu.VMEM((size, chans), F32), pltpu.VMEM((peers, cut, chans), F32)],
    )
    terms = [cuts[0]] + [lax.ppermute(cuts[k], "row", flip("row", k)) for k in range(1, peers)]
    scale = 1.0 / math.sqrt(images * height * cols)
    one, two = call(functools.partial(last_kernel, peers, scale), [((2 * cut, 128), F32)] * 2, tuple(terms))
    return (result[0].reshape(features.shape), one.reshape(-1), two.reshape(-1))


def solution(mesh):
    placed = (P("img", "row", None, None), P("img", "row", None, None), P(), P())
    return jax.shard_map(
        local_part,
        mesh=mesh,
        in_specs=placed,
        out_specs=(P("img", "row", None, None), P(("img", "row")), P(("img", "row"))),
        check_vma=False,
    )
```
